16 devices in a mesh: dp: 1, ep: 16 (over x, y, z, core).
Axes of the slice: x: 2, y: 2, z: 2, core: 2. Of those that a mesh axis runs over, the one named last changes fastest.
Arguments:
- x: bfloat16 [1, 16, 256, 2560], P('dp', 'ep')
- expert: int32 [1, 16, 256, 6], P('dp', 'ep')
- slot: int32 [1, 16, 256, 6], P('dp', 'ep')
- gate: float32 [1, 16, 256, 6], P('dp', 'ep')
- w_gate: bfloat16 [80, 2560, 1536], P('ep')
- w_up: bfloat16 [80, 2560, 1536], P('ep')
- w_down: bfloat16 [80, 1536, 2560], P('ep')
- s_gate: bfloat16 [2560, 3072], replicated
- s_up: bfloat16 [2560, 3072], replicated
- s_down: bfloat16 [3072, 2560], replicated
Outputs:
- y: bfloat16 [1, 16, 256, 2560], P('dp', 'ep')
All inputs are finite; a program needn't handle non-finite values.
Results may differ from the reference program's by a relative error of at most 0.009.
Values are sent between devices in bfloat16 or wider.
A program may use at most 2 GiB of HBM per device.

```python
import jax
import jax.numpy as jnp

MEMBERS = 16
TOKENS = 256
D = 2560
FF = 1536
TOP = 6
EXPERTS = 80
SHARED_FF = 3072
SLOTS = 5 * TOKENS * TOP // (4 * EXPERTS)


def setup_inputs(seed: int = 0, part: int = 0) -> dict:
    own, k1, k2, k3, k4, k5, k6 = jax.random.split(jax.random.key(seed), 7)
    kx, ke, kl, kg = jax.random.split(jax.random.fold_in(own, part), 4)
    devices = (1, MEMBERS)
    place = jax.random.permutation(kl, jnp.arange(EXPERTS, dtype=jnp.uint32))
    slow = ((EXPERTS + (9 * place) % EXPERTS) << ((9 * place) // EXPERTS)) // EXPERTS
    wait = (jax.random.bits(ke, (*devices, TOKENS, EXPERTS), jnp.uint32) >> 10) * slow
    expert = jnp.argsort(wait, axis=-1)[..., :TOP].astype(jnp.int32)
    chosen = jax.nn.one_hot(expert, EXPERTS, dtype=jnp.int32)
    in_line = jnp.cumsum(chosen.reshape(*devices, TOKENS * TOP, EXPERTS), axis=2) - 1
    slot = jnp.sum(in_line.reshape(chosen.shape) * chosen, axis=-1)

    def one(key, rows, columns):
        return (jax.random.normal(key, (rows, columns), jnp.float32) * rows**-0.5).astype(jnp.bfloat16)

    def weights(key, rows, columns):
        return jax.lax.map(lambda k: one(k, rows, columns), jax.random.split(key, EXPERTS))

    return {
        "x": jax.random.normal(kx, (*devices, TOKENS, D), jnp.float32).astype(jnp.bfloat16),
        "expert": expert,
        "slot": slot,
        "gate": jax.nn.softmax(jax.random.normal(kg, expert.shape, jnp.float32)),
        "w_gate": weights(k1, D, FF),
        "w_up": weights(k2, D, FF),
        "w_down": weights(k3, FF, D),
        "s_gate": one(k4, D, SHARED_FF),
        "s_up": one(k5, D, SHARED_FF),
        "s_down": one(k6, SHARED_FF, D),
    }


def einsum(form, a, b):
    return jnp.einsum(form, a.astype(jnp.float32), b.astype(jnp.float32))


def for_all(x, s_gate, s_up, s_down):
    h = jax.nn.silu(einsum("...d,df->...f", x, s_gate)) * einsum("...d,df->...f", x, s_up)
    return einsum("...f,fd->...d", h.astype(jnp.bfloat16), s_down)


def reference(x, expert, slot, gate, w_gate, w_up, w_down, s_gate, s_up, s_down):
    to_expert = jax.nn.one_hot(expert, EXPERTS, dtype=jnp.bfloat16)
    to_slot = jax.nn.one_hot(slot, SLOTS, dtype=jnp.bfloat16)
    weighted = to_expert * gate[..., None].astype(jnp.bfloat16)
    dispatch = einsum("abtke,abtkc->abtec", to_expert, to_slot).astype(jnp.bfloat16)
    combine = einsum("abtke,abtkc->abtec", weighted, to_slot).astype(jnp.bfloat16)
    z = einsum("abtec,abtd->aebcd", dispatch, x).astype(jnp.bfloat16)
    h = jax.nn.silu(einsum("aebcd,edf->aebcf", z, w_gate))
    h = (h * einsum("aebcd,edf->aebcf", z, w_up)).astype(jnp.bfloat16)
    out = einsum("aebcf,efd->aebcd", h, w_down).astype(jnp.bfloat16)
    y = einsum("abtec,aebcd->abtd", combine, out)
    return (y + for_all(x, s_gate, s_up, s_down)).astype(jnp.bfloat16)
```

```python
import functools

import jax
import jax.numpy as jnp
from jax import lax
from jax.experimental import pallas as pl
from jax.experimental.pallas import tpu as pltpu
from jax.sharding import PartitionSpec as P

MESH = pl.DeviceIdType.MESH
BF = jnp.bfloat16
F32 = jnp.float32
DC = 256
BITS = (4, 2, 1)
PARTS = ((0, 96), (96, 80), (176, 80))
RING = 4
DROPPED = 128


def axes(me):
    def flip(bit):
        return me + bit * (1 - 2 * lax.rem(lax.div(me, bit), 2))

    return [flip(2 * b) for b in BITS], flip(1)


def meet(links, twin):
    barrier = pltpu.get_barrier_semaphore()
    for other in (*links, twin):
        pl.semaphore_signal(barrier, inc=1, device_id={"ep": other}, device_id_type=MESH)
    pl.semaphore_wait(barrier, 4)


def silu_mul(g, u):
    return (g * jax.nn.sigmoid(g) * u).astype(BF)


def up_kernel(x_ref, m_ref, wg, wu, sg, su, h_out, hs_out, cm_out,
              xr, mr, dm, cm, zs, ag, au, wb, hb, hsb, ss, rs, wsem, osem):
    me = lax.axis_index("ep")
    links, twin = axes(me)
    nc = xr.shape[0]
    experts, rows, ff = ag.shape
    tokens = x_ref.shape[0]
    slots = rows // 16
    n_shared = 2 * nc
    n_steps = n_shared + nc * experts

    def start_w(s):
        slot = lax.rem(s, RING)

        @pl.when(s < n_shared)
        def _():
            half, k = lax.div(s, nc), lax.rem(s, nc)
            at = (pl.ds(pl.multiple_of(k * DC, DC), DC), pl.ds(pl.multiple_of(half * ff, ff), ff))
            for i, w in enumerate((sg, su)):
                pltpu.make_async_copy(w.at[at], wb.at[slot, i], wsem.at[slot, i]).start()

        @pl.when((s >= n_shared) & (s < n_steps))
        def _():
            k, e = lax.div(s - n_shared, experts), lax.rem(s - n_shared, experts)
            for i, w in enumerate((wg, wu)):
                src = w.at[e, pl.ds(pl.multiple_of(k * DC, DC), DC), :]
                pltpu.make_async_copy(src, wb.at[slot, i], wsem.at[slot, i]).start()

    def wait_w(s):
        slot = lax.rem(s, RING)
        for i, w in enumerate((wg, wu)):
            pltpu.make_async_copy(w.at[0, pl.ds(0, DC), :], wb.at[slot, i], wsem.at[slot, i]).wait()
        return slot

    for s in range(RING):
        start_w(s)
    meet(links, twin)

    def copy(kind, i, k):
        row = nc if k is None else k
        own = m_ref if k is None else x_ref.at[:, pl.ds(pl.multiple_of(k * DC, DC), DC)]

        def block(slot):
            return mr.at[slot] if k is None else xr.at[k, slot]

        if kind == "D":
            src, dst, to, n = own, block(2 * BITS[i]), links[i], i
        elif kind == "F":
            src, dst = block(2 * BITS[(i + 1) % 3]), block(2 * (BITS[i] | BITS[(i + 1) % 3]))
            to, n = links[i], 3 + i
        elif kind == "G":
            part = pl.ds(*PARTS[i])
            src = block(2 * (BITS[(i + 1) % 3] | BITS[(i + 2) % 3])).at[part]
            dst, to, n = block(14).at[part], links[i], 6 + i
        else:
            src, dst, to, n = own if i == 0 else block(2 * i), block(2 * i + 1), twin, 9 + i
        return pltpu.make_async_remote_copy(
            src_ref=src, dst_ref=dst, send_sem=ss.at[row, n], recv_sem=rs.at[row, n],
            device_id={"ep": to}, device_id_type=MESH)

    def both(k, do):
        @pl.when(k == 0)
        def _():
            do(None)

        do(k)

    def first(k):
        for i in range(3):
            copy("D", i, k).start()

    def second(k):
        for i in range(3):
            copy("D", i, k).wait_recv()
            copy("F", (i + 2) % 3, k).start()
            copy("S", BITS[i], k).start()

    def third(k):
        for i in range(3):
            copy("F", i, k).wait_recv()
            copy("G", (i + 2) % 3, k).start()
            copy("S", BITS[i] | BITS[(i + 1) % 3], k).start()

    def fourth(k):
        for i in range(3):
            copy("G", i, k).wait_recv()
        copy("S", 7, k).start()

    def arrive(k):
        for q in range(8):
            copy("S", q, k).wait_recv()

    def leave(k):
        for kind, count in (("D", 3), ("F", 3), ("G", 3), ("S", 8)):
            for i in range(count):
                copy(kind, i, k).wait_send()

    first(None)
    for k in range(3):
        first(k)
    copy("S", 0, None).start()

    @pl.loop(0, nc)
    def _(k):
        copy("S", 0, k).start()
        xr[k, 0] = x_ref[:, pl.ds(pl.multiple_of(k * DC, DC), DC)]

    mr[0] = m_ref[...]

    def matmul(lhs, slot, e, m, fresh):
        for n in range(ff // 256):
            cols = slice(256 * n, 256 * (n + 1))
            for i, acc in enumerate((ag, au)):
                old = jnp.where(fresh, 0.0, acc[e, :m, cols])
                acc[e, :m, cols] = old + jnp.dot(lhs, wb[slot, i, :, cols], preferred_element_type=F32)

    def shared_step(s):
        slot = wait_w(s)
        half, k = lax.div(s, nc), lax.rem(s, nc)
        matmul(xr[k, 0], slot, 0, tokens, k == 0)
        start_w(s + RING)

        @pl.when(k == nc - 1)
        def _():
            for n in range(ff // 256):
                cols = slice(256 * n, 256 * (n + 1))
                at = pl.ds(pl.multiple_of(half * ff + 256 * n, 256), 256)
                hsb[:, at] = silu_mul(ag[0, :tokens, cols], au[0, :tokens, cols])

    def masks():
        base = (me * (experts * slots)).astype(F32)
        lane = lax.broadcasted_iota(jnp.int32, (tokens, 128), 1)
        want = jnp.where(lane < experts * slots, lane.astype(F32) + base, -1.0)

        @pl.loop(0, 16)
        def _(d):
            m = mr[d].astype(F32)
            hit = jnp.zeros((tokens, 128), F32)
            weight = jnp.zeros((tokens, 128), F32)
            for j in range(6):
                place = m[:, j:j + 1] * float(slots) + m[:, 6 + j:7 + j]
                same = place == want
                hit = jnp.where(same, 1.0, hit)
                weight = jnp.where(same, m[:, 12 + j:13 + j], weight)
            dm[d] = hit.T.astype(BF)
            cm[d] = weight.astype(BF)

    def dispatch(k):
        @pl.loop(0, 16)
        def _(d):
            z = jnp.dot(dm[d], xr[k, d], preferred_element_type=F32)
            for e in range(experts):
                zs[e, pl.ds(pl.multiple_of(d * slots, 8), slots), :] = z[e * slots:(e + 1) * slots]

    def out_copy(e):
        return pltpu.make_async_copy(hb.at[lax.rem(e, 2)], h_out.at[e], osem.at[lax.rem(e, 2)])

    def expert_step(k, e):
        s = n_shared + k * experts + e
        slot = wait_w(s)
        matmul(zs[e].astype(BF), slot, e, rows, k == 0)
        start_w(s + RING)

        @pl.when(k == nc - 1)
        def _():
            @pl.when(e >= 2)
            def _():
                out_copy(e - 2).wait()

            for n in range(ff // 256):
                cols = slice(256 * n, 256 * (n + 1))
                hb[lax.rem(e, 2), :, cols] = silu_mul(ag[e, :, cols], au[e, :, cols])
            out_copy(e).start()

    hs_copy = pltpu.make_async_copy(hsb, hs_out, osem.at[2])
    cm_copy = pltpu.make_async_copy(cm, cm_out, osem.at[3])
    per_tick = n_shared // 4

    @pl.loop(0, nc + 4)
    def _(t):
        @pl.when(t < nc)
        def _():
            both(t, second)

        @pl.when((t >= 2) & (t < nc + 2))
        def _():
            both(t - 2, third)

        @pl.when(t + 3 < nc)
        def _():
            first(t + 3)

        @pl.when(t < 4)
        def _():
            @pl.loop(0, per_tick)
            def _(j):
                shared_step(t * per_tick + j)

        @pl.when(t == 4)
        def _():
            hs_copy.start()

        @pl.when(t >= 4)
        def _():
            k = t - 4
            both(k, fourth)
            both(k, arrive)

            @pl.when(k == 0)
            def _():
                masks()
                cm_copy.start()

            dispatch(k)

            @pl.loop(0, experts)
            def _(e):
                expert_step(k, e)

    out_copy(experts - 2).wait()
    out_copy(experts - 1).wait()
    hs_copy.wait()
    cm_copy.wait()
    leave(None)

    @pl.loop(0, nc)
    def _(k):
        leave(k)


def down_kernel(h_in, hs_in, cm_in, wd, sd, y_ref, hv, hsv, cmv, wb, os, sums, mine, p1, rd,
                sa, ra, sb, rb, sc, rc, lsem, wsem, ss, rs):
    me = lax.axis_index("ep")
    links, twin = axes(me)
    nc = rd.shape[0]
    experts, rows, ff = hv.shape
    slots = rows // 16
    tokens = y_ref.shape[0]
    tiles = experts + 2
    n_steps = nc * tiles

    def start_w(s):
        slot = lax.rem(s, RING)
        j, t = lax.div(s, tiles), lax.rem(s, tiles)
        cols = pl.ds(pl.multiple_of(j * DC, DC), DC)

        @pl.when((s < n_steps) & (t < experts))
        def _():
            pltpu.make_async_copy(wd.at[t, :, cols], wb.at[slot], wsem.at[slot]).start()

        @pl.when((s < n_steps) & (t >= experts))
        def _():
            part = pl.ds(pl.multiple_of((t - experts) * ff, ff), ff)
            pltpu.make_async_copy(sd.at[part, cols], wb.at[slot], wsem.at[slot]).start()

    def wait_w(s):
        slot = lax.rem(s, RING)
        pltpu.make_async_copy(wd.at[0, :, pl.ds(0, DC)], wb.at[slot], wsem.at[slot]).wait()
        return slot

    loads = [pltpu.make_async_copy(h_in.at[e], hv.at[e], lsem.at[e]) for e in range(experts)]
    loads += [pltpu.make_async_copy(cm_in, cmv, lsem.at[experts]),
              pltpu.make_async_copy(hs_in, hsv, lsem.at[experts + 1])]
    loads[0].start()
    for s in range(RING):
        start_w(s)
    for c in loads[1:]:
        c.start()
    meet(links, twin)

    def copy(kind, i, k):
        if kind == "P":
            src, dst, to, n = p1.at[lax.rem(k, 3)], rd.at[k], twin, 0
        elif kind == "A":
            part = pl.ds(*PARTS[i])
            src, dst, to, n = sa.at[k, part], ra.at[k, part], links[i], 1 + i
        elif kind == "B":
            src, dst, to, n = sb.at[k, i], rb.at[k, i], links[i], 4 + i
        else:
            src, dst, to, n = sc.at[k, i], rc.at[k, i], links[i], 7 + i
        return pltpu.make_async_remote_copy(
            src_ref=src, dst_ref=dst, send_sem=ss.at[k, n], recv_sem=rs.at[k, n],
            device_id={"ep": to}, device_id_type=MESH)

    for c in loads:
        c.wait()

    def project(k):
        @pl.loop(0, experts)
        def _(e):
            s = k * tiles + e
            slot = wait_w(s)
            os[e] = jnp.dot(hv[e], wb[slot], preferred_element_type=F32)
            start_w(s + RING)

    def partial(d):
        o = [os[e, pl.ds(pl.multiple_of(d * slots, 8), slots), :] for e in range(experts)]
        o.append(jnp.zeros((128 - experts * slots, DC), F32))
        return jnp.dot(cmv[d], jnp.concatenate(o, axis=0).astype(BF), preferred_element_type=F32)

    def combine(k):
        slot = lax.rem(k, 3)

        @pl.when(k >= 3)
        def _():
            copy("P", 0, k - 3).wait_send()

        @pl.loop(0, 8)
        def _(q):
            p1[slot, q] = partial(2 * q + 1).astype(BF)

        copy("P", 0, k).start()

        @pl.loop(1, 8)
        def _(q):
            sums[slot, q - 1] = partial(2 * q)

        mine[k] = partial(0)

    def shared(k):
        s = k * tiles + experts
        for half in range(2):
            slot = wait_w(s + half)
            mine[k] += jnp.dot(hsv[:, half * ff:(half + 1) * ff], wb[slot], preferred_element_type=F32)
            start_w(s + half + RING)

    def stage_a(k):
        slot = lax.rem(k, 3)
        copy("P", 0, k).wait_recv()
        sa[k] = (sums[slot, 6] + rd[k, 7].astype(F32)).astype(BF)
        for i in range(3):
            copy("A", i, k).start()

        @pl.loop(1, 7)
        def _(q):
            sums[slot, q - 1] += rd[k, q].astype(F32)

        mine[k] += rd[k, 0].astype(F32)

    def stage_b(k):
        slot = lax.rem(k, 3)
        for i in range(3):
            copy("A", i, k).wait_recv()
            b, q = (i + 1) % 3, 7 ^ BITS[i]
            for p, (start, size) in enumerate(PARTS):
                part = slice(start, start + size)
                v = sums[slot, q - 1, part]
                if p == i:
                    v = v + ra[k, part].astype(F32)
                sb[k, b, part] = v.astype(BF)
            copy("B", b, k).start()

    def stage_c(k):
        slot = lax.rem(k, 3)
        for i in range(3):
            copy("B", i, k).wait_recv()
            c = (i + 1) % 3
            sc[k, c] = (sums[slot, BITS[c] - 1] + rb[k, i].astype(F32)).astype(BF)
            copy("C", c, k).start()

    def finish(k):
        total = mine[k]
        for i in range(3):
            copy("C", i, k).wait_recv()
            total += rc[k, i].astype(F32)
        y_ref[:, pl.ds(pl.multiple_of(k * DC, DC), DC)] = total.astype(BF)

    @pl.loop(0, nc + 5)
    def _(t):
        @pl.when(t < nc)
        def _():
            project(t)

        @pl.when((t >= 1) & (t < nc + 1))
        def _():
            stage_a(t - 1)

        @pl.when((t >= 2) & (t < nc + 2))
        def _():
            stage_b(t - 2)

        @pl.when((t >= 3) & (t < nc + 3))
        def _():
            stage_c(t - 3)

        @pl.when(t < nc)
        def _():
            combine(t)
            shared(t)

        @pl.when(t >= 5)
        def _():
            finish(t - 5)

    @pl.loop(0, nc)
    def _(k):
        @pl.when(k >= nc - 3)
        def _():
            copy("P", 0, k).wait_send()

        for kind in "ABC":
            for i in range(3):
                copy(kind, i, k).wait_send()


def solution(mesh):
    def local(x, expert, slot, gate, w_gate, w_up, w_down, s_gate, s_up, s_down):
        x, expert, slot, gate = x[0, 0], expert[0, 0], slot[0, 0], gate[0, 0]
        tokens, d = x.shape
        top = expert.shape[1]
        experts, _, ff = w_gate.shape
        slots = 5 * tokens * top // (4 * experts * 16)
        rows, nc = 16 * slots, d // DC
        kept = slot < slots
        meta = jnp.concatenate([
            jnp.where(kept, expert, DROPPED).astype(BF), jnp.where(kept, slot, 0).astype(BF), gate.astype(BF),
            jnp.zeros((tokens, 128 - 3 * top), BF)], axis=1)
        dma = pltpu.SemaphoreType.DMA
        vmem = pl.BlockSpec(memory_space=pltpu.VMEM)
        hbm = pl.BlockSpec(memory_space=pl.ANY)
        h, hs, cm = pl.pallas_call(
            up_kernel,
            name="up",
            out_shape=[jax.ShapeDtypeStruct((experts, rows, ff), BF),
                       jax.ShapeDtypeStruct((tokens, 2 * ff), BF),
                       jax.ShapeDtypeStruct((16, tokens, 128), BF)],
            in_specs=[vmem, vmem, hbm, hbm, hbm, hbm],
            out_specs=[hbm, hbm, hbm],
            scratch_shapes=[
                pltpu.VMEM((nc, 16, tokens, DC), BF), pltpu.VMEM((16, tokens, 128), BF),
                pltpu.VMEM((16, 128, tokens), BF), pltpu.VMEM((16, tokens, 128), BF),
                pltpu.VMEM((experts, rows, DC), F32),
                pltpu.VMEM((experts, rows, ff), F32), pltpu.VMEM((experts, rows, ff), F32),
                pltpu.VMEM((RING, 2, DC, ff), BF), pltpu.VMEM((2, rows, ff), BF),
                pltpu.VMEM((tokens, 2 * ff), BF),
                dma((nc + 1, 17)), dma((nc + 1, 17)), dma((RING, 2)), dma((4,))],
            compiler_params=pltpu.CompilerParams(
                collective_id=0, has_side_effects=True, vmem_limit_bytes=67_043_328),
        )(x, meta, w_gate, w_up, s_gate, s_up)
        y = pl.pallas_call(
            down_kernel,
            name="down",
            out_shape=jax.ShapeDtypeStruct((tokens, d), BF),
            in_specs=[hbm] * 5,
            out_specs=vmem,
            scratch_shapes=[
                pltpu.VMEM((experts, rows, ff), BF), pltpu.VMEM((tokens, 2 * ff), BF),
                pltpu.VMEM((16, tokens, 128), BF), pltpu.VMEM((RING, ff, DC), BF),
                pltpu.VMEM((experts, rows, DC), F32), pltpu.VMEM((3, 7, tokens, DC), F32),
                pltpu.VMEM((nc, tokens, DC), F32), pltpu.VMEM((3, 8, tokens, DC), BF),
                pltpu.VMEM((nc, 8, tokens, DC), BF),
                pltpu.VMEM((nc, tokens, DC), BF), pltpu.VMEM((nc, tokens, DC), BF),
                pltpu.VMEM((nc, 3, tokens, DC), BF), pltpu.VMEM((nc, 3, tokens, DC), BF),
                pltpu.VMEM((nc, 3, tokens, DC), BF), pltpu.VMEM((nc, 3, tokens, DC), BF),
                dma((experts + 2,)), dma((RING,)), dma((nc, 10)), dma((nc, 10))],
            compiler_params=pltpu.CompilerParams(
                collective_id=1, has_side_effects=True, vmem_limit_bytes=67_043_328),
        )(h, hs, cm, w_down, s_down)
        return y[None, None]

    tok = P("dp", "ep", None, None)
    return jax.shard_map(
        local, mesh=mesh,
        in_specs=(tok, tok, tok, tok, P("ep"), P("ep"), P("ep"), P(), P(), P()),
        out_specs=tok, check_vma=False)
```

```python
import functools

import jax
import jax.numpy as jnp
from jax import lax
from jax.experimental import pallas as pl
from jax.experimental.pallas import tpu as pltpu
from jax.sharding import PartitionSpec as P

MESH = pl.DeviceIdType.MESH
BF = jnp.bfloat16
F32 = jnp.float32
DC = 256
BITS = (4, 2, 1)
PARTS = ((0, 96), (96, 80), (176, 80))
RING = 3
RING2 = 8
KC = 2 * DC
DROPPED = 128


def axes(me):
    def flip(bit):
        return me + bit * (1 - 2 * lax.rem(lax.div(me, bit), 2))

    return [flip(2 * b) for b in BITS], flip(1)


def meet(links, twin):
    barrier = pltpu.get_barrier_semaphore()
    for other in (*links, twin):
        pl.semaphore_signal(barrier, inc=1, device_id={"ep": other}, device_id_type=MESH)
    pl.semaphore_wait(barrier, 4)


def silu_mul(g, u):
    return (g * jax.nn.sigmoid(g) * u).astype(BF)


def up_kernel(x_ref, m_ref, wg, wu, sg, su, h_out, hs_out, cm_out,
              xr, mr, dm, cm, zs, ag, au, wb, hb, hsb, ss, rs, wsem, osem):
    me = lax.axis_index("ep")
    links, twin = axes(me)
    nc = xr.shape[0]
    experts, rows, ff = ag.shape
    tokens = x_ref.shape[0]
    slots = rows // 16
    np_ = nc // 2
    n_shared = 2 * np_
    n_steps = n_shared + np_ * experts

    def start_w(s):
        slot = lax.rem(s, RING)

        @pl.when(s < n_shared)
        def _():
            half, k = lax.div(s, np_), lax.rem(s, np_)
            at = (pl.ds(pl.multiple_of(k * KC, KC), KC), pl.ds(pl.multiple_of(half * ff, ff), ff))
            for i, w in enumerate((sg, su)):
                pltpu.make_async_copy(w.at[at], wb.at[slot, i], wsem.at[slot, i]).start()

        @pl.when((s >= n_shared) & (s < n_steps))
        def _():
            k, e = lax.div(s - n_shared, experts), lax.rem(s - n_shared, experts)
            for i, w in enumerate((wg, wu)):
                src = w.at[e, pl.ds(pl.multiple_of(k * KC, KC), KC), :]
                pltpu.make_async_copy(src, wb.at[slot, i], wsem.at[slot, i]).start()

    def wait_w(s):
        slot = lax.rem(s, RING)
        for i, w in enumerate((wg, wu)):
            pltpu.make_async_copy(w.at[0, pl.ds(0, KC), :], wb.at[slot, i], wsem.at[slot, i]).wait()
        return slot

    for s in range(RING):
        start_w(s)
    meet(links, twin)

    def copy(kind, i, k):
        row = nc if k is None else k
        own = m_ref if k is None else x_ref.at[:, pl.ds(pl.multiple_of(k * DC, DC), DC)]

        def block(slot):
            return mr.at[slot] if k is None else xr.at[k, slot]

        if kind == "D":
            src, dst, to, n = own, block(2 * BITS[i]), links[i], i
        elif kind == "F":
            src, dst = block(2 * BITS[(i + 1) % 3]), block(2 * (BITS[i] | BITS[(i + 1) % 3]))
            to, n = links[i], 3 + i
        elif kind == "G":
            src, dst = block(2 * (BITS[(i + 1) % 3] | BITS[(i + 2) % 3])), block(14)
            if k is not None:
                src, dst = src.at[pl.ds(*PARTS[i])], dst.at[pl.ds(*PARTS[i])]
            to, n = links[i], 6 + i
        else:
            src, dst, to, n = own if i == 0 else block(2 * i), block(2 * i + 1), twin, 9 + i
        return pltpu.make_async_remote_copy(
            src_ref=src, dst_ref=dst, send_sem=ss.at[row, n], recv_sem=rs.at[row, n],
            device_id={"ep": to}, device_id_type=MESH)

    def first(k):
        for i in range(3):
            copy("D", i, k).start()

    def second(k):
        for i in range(3):
            copy("D", i, k).wait_recv()
            copy("F", (i + 2) % 3, k).start()
            copy("S", BITS[i], k).start()

    def whole(k, i):
        return k is not None or i == 0

    def third(k):
        for i in range(3):
            copy("F", i, k).wait_recv()
            if whole(k, (i + 2) % 3):
                copy("G", (i + 2) % 3, k).start()
            copy("S", BITS[i] | BITS[(i + 1) % 3], k).start()

    def fourth(k):
        for i in range(3):
            if whole(k, i):
                copy("G", i, k).wait_recv()
        copy("S", 7, k).start()

    def arrive(k):
        for q in range(8):
            copy("S", q, k).wait_recv()

    def leave(k):
        for kind, count in (("D", 3), ("F", 3), ("G", 3), ("S", 8)):
            for i in range(count):
                if kind != "G" or whole(k, i):
                    copy(kind, i, k).wait_send()

    first(None)
    for k in range(2):
        first(k)
    copy("S", 0, None).start()

    @pl.loop(0, nc)
    def _(k):
        copy("S", 0, k).start()
        xr[k, 0] = x_ref[:, pl.ds(pl.multiple_of(k * DC, DC), DC)]

    mr[0] = m_ref[...]

    def matmul(lhs, slot, e, k, emit):
        m = lhs.shape[0]

        def dots(cols):
            return [jnp.dot(lhs, wb[slot, i, :, cols], preferred_element_type=F32) for i in range(2)]

        tiles = [(n, slice(256 * n, 256 * (n + 1))) for n in range(ff // 256)]

        @pl.when(k == 0)
        def _():
            for n, cols in tiles:
                ag[e, :m, cols], au[e, :m, cols] = dots(cols)

        @pl.when((k > 0) & (k < np_ - 1))
        def _():
            for n, cols in tiles:
                g, u = dots(cols)
                ag[e, :m, cols] += g
                au[e, :m, cols] += u

        @pl.when(k == np_ - 1)
        def _():
            for n, cols in tiles:
                g, u = dots(cols)
                emit(n, silu_mul(ag[e, :m, cols] + g, au[e, :m, cols] + u))

    def shared_step(s):
        slot = wait_w(s)
        half, k = lax.div(s, np_), lax.rem(s, np_)

        def emit(n, v):
            hsb[:, pl.ds(pl.multiple_of(half * ff + 256 * n, 256), 256)] = v

        matmul(x_ref[:, pl.ds(pl.multiple_of(k * KC, KC), KC)], slot, 0, k, emit)
        start_w(s + RING)

    def masks():
        base = (me * (experts * slots)).astype(F32)
        row = lax.broadcasted_iota(jnp.int32, (128, tokens), 0)
        want = jnp.where(row < experts * slots, row.astype(F32) + base, -1.0)

        @pl.loop(0, 16)
        def _(d):
            m = mr[d].astype(F32)
            hit = jnp.zeros((128, tokens), F32)
            weight = jnp.zeros((128, tokens), F32)
            for j in range(6):
                place = m[j:j + 1] * float(slots) + m[6 + j:7 + j]
                same = place == want
                hit = jnp.where(same, 1.0, hit)
                weight = jnp.where(same, m[12 + j:13 + j], weight)
            dm[d] = hit.astype(BF)
            cm[d] = weight.T.astype(BF)

    def dispatch(p):
        for half in range(2):
            cols = slice(half * DC, (half + 1) * DC)
            for q in range(8):
                z = [jnp.dot(dm[2 * q + c], xr[2 * p + half, 2 * q + c], preferred_element_type=F32) for c in range(2)]
                for e in range(experts):
                    pair = [v[e * slots:(e + 1) * slots] for v in z]
                    zs[e, 2 * q * slots:2 * (q + 1) * slots, cols] = jnp.concatenate(pair, axis=0).astype(BF)

    def out_copy(e):
        return pltpu.make_async_copy(hb.at[lax.rem(e, 2)], h_out.at[e], osem.at[lax.rem(e, 2)])

    def expert_step(p, e):
        s = n_shared + p * experts + e
        slot = wait_w(s)

        @pl.when((p == np_ - 1) & (e >= 2))
        def _():
            out_copy(e - 2).wait()

        def emit(n, v):
            hb[lax.rem(e, 2), :, 256 * n:256 * (n + 1)] = v

        matmul(zs[e], slot, e, p, emit)
        start_w(s + RING)

        @pl.when(p == np_ - 1)
        def _():
            out_copy(e).start()

    hs_copy = pltpu.make_async_copy(hsb, hs_out, osem.at[2])
    cm_copy = pltpu.make_async_copy(cm, cm_out, osem.at[3])
    split = 2

    @pl.loop(0, nc + 4)
    def _(t):
        for step, do in enumerate((second, third, fourth)):
            @pl.when(t == step)
            def _():
                do(None)

        @pl.when(t < nc)
        def _():
            second(t)

        @pl.when((t >= 1) & (t < nc + 1))
        def _():
            third(t - 1)

        @pl.when(t + 2 < nc)
        def _():
            first(t + 2)

        @pl.when((t >= 2) & (t < nc + 2))
        def _():
            fourth(t - 2)

        @pl.when(t == 3)
        def _():
            hs_copy.start()
            cm_copy.start()

        @pl.when(t < 3)
        def _():
            @pl.loop(0, 4)
            def _(j):
                @pl.when(4 * t + j < n_shared)
                def _():
                    shared_step(4 * t + j)

        @pl.when(t == 2)
        def _():
            arrive(None)
            masks()

        p = lax.div(t - 3, 2)
        early = lax.rem(t, 2) == 1

        @pl.when((t >= 3) & (t < nc + 3) & early)
        def _():
            arrive(2 * p)
            arrive(2 * p + 1)
            dispatch(p)

            @pl.loop(0, split)
            def _(e):
                expert_step(p, e)

        @pl.when((t >= 4) & (t < nc + 4) & ~early)
        def _():
            @pl.loop(split, experts)
            def _(e):
                expert_step(p, e)

    out_copy(experts - 2).wait()
    out_copy(experts - 1).wait()
    hs_copy.wait()
    cm_copy.wait()
    leave(None)

    @pl.loop(0, nc)
    def _(k):
        leave(k)


def down_kernel(h_in, hs_in, cm_in, wd, sd, y_ref, hv, hsv, cmv, wb, os, sums, mine, p1, rd,
                sa, ra, sb, rb, sc, rc, lsem, wsem, ss, rs):
    me = lax.axis_index("ep")
    links, twin = axes(me)
    nc = rd.shape[0]
    experts, rows, ff = hv.shape
    slots = rows // 16
    tokens = y_ref.shape[0]
    tiles = experts + 2
    n_steps = nc * tiles

    def start_w(s):
        slot = lax.rem(s, RING2)
        j, t = lax.div(s, tiles), lax.rem(s, tiles)
        cols = pl.ds(pl.multiple_of(j * DC, DC), DC)

        @pl.when((s < n_steps) & (t < experts))
        def _():
            pltpu.make_async_copy(wd.at[t, :, cols], wb.at[slot], wsem.at[slot]).start()

        @pl.when((s < n_steps) & (t >= experts))
        def _():
            part = pl.ds(pl.multiple_of((t - experts) * ff, ff), ff)
            pltpu.make_async_copy(sd.at[part, cols], wb.at[slot], wsem.at[slot]).start()

    def wait_w(s):
        slot = lax.rem(s, RING2)
        pltpu.make_async_copy(wd.at[0, :, pl.ds(0, DC)], wb.at[slot], wsem.at[slot]).wait()
        return slot

    loads = [pltpu.make_async_copy(h_in.at[e], hv.at[e], lsem.at[e]) for e in range(experts)]
    loads += [pltpu.make_async_copy(cm_in, cmv, lsem.at[experts]),
              pltpu.make_async_copy(hs_in, hsv, lsem.at[experts + 1])]
    loads[0].start()
    for s in range(RING2):
        start_w(s)
    for c in loads[1:]:
        c.start()
    meet(links, twin)

    def copy(kind, i, k):
        if kind == "P":
            src, dst, to, n = p1.at[lax.rem(k, 3)], rd.at[k], twin, 0
        elif kind == "A":
            part = pl.ds(*PARTS[i])
            src, dst, to, n = sa.at[k, part], ra.at[k, part], links[i], 1 + i
        elif kind == "B":
            src, dst, to, n = sb.at[k, i], rb.at[k, i], links[i], 4 + i
        else:
            src, dst, to, n = sc.at[k, i], rc.at[k, i], links[i], 7 + i
        return pltpu.make_async_remote_copy(
            src_ref=src, dst_ref=dst, send_sem=ss.at[k, n], recv_sem=rs.at[k, n],
            device_id={"ep": to}, device_id_type=MESH)

    for c in loads:
        c.wait()

    def project(k):
        held = [wait_w(k * tiles + e) for e in range(experts)]
        for e, slot in enumerate(held):
            os[e] = jnp.dot(hv[e], wb[slot], preferred_element_type=F32)
        for e in range(experts):
            start_w(k * tiles + e + RING2)

    def partial(d):
        o = [os[e, d * slots:(d + 1) * slots, :] for e in range(experts)]
        o.append(jnp.zeros((128 - experts * slots, DC), F32))
        return jnp.dot(cmv[d], jnp.concatenate(o, axis=0).astype(BF), preferred_element_type=F32)

    def combine(k):
        slot = lax.rem(k, 3)

        @pl.when(k >= 3)
        def _():
            copy("P", 0, k - 3).wait_send()

        for q in range(8):
            p1[slot, q] = partial(2 * q + 1).astype(BF)

        copy("P", 0, k).start()

        for q in range(1, 8):
            sums[slot, q - 1] = partial(2 * q)

        mine[k] = partial(0)

    def shared(k):
        held = [wait_w(k * tiles + experts + half) for half in range(2)]
        mine[k] += sum(jnp.dot(hsv[:, half * ff:(half + 1) * ff], wb[slot], preferred_element_type=F32)
                       for half, slot in enumerate(held))
        for half in range(2):
            start_w(k * tiles + experts + half + RING2)

    def stage_a(k):
        slot = lax.rem(k, 3)
        copy("P", 0, k).wait_recv()
        sa[k] = (sums[slot, 6] + rd[k, 7].astype(F32)).astype(BF)
        for i in range(3):
            copy("A", i, k).start()

        @pl.loop(1, 7)
        def _(q):
            sums[slot, q - 1] += rd[k, q].astype(F32)

        mine[k] += rd[k, 0].astype(F32)

    def stage_b(k):
        slot = lax.rem(k, 3)
        for i in range(3):
            copy("A", i, k).wait_recv()
            b, q = (i + 1) % 3, 7 ^ BITS[i]
            for p, (start, size) in enumerate(PARTS):
                part = slice(start, start + size)
                v = sums[slot, q - 1, part]
                if p == i:
                    v = v + ra[k, part].astype(F32)
                sb[k, b, part] = v.astype(BF)
            copy("B", b, k).start()

    def stage_c(k):
        slot = lax.rem(k, 3)
        for i in range(3):
            copy("B", i, k).wait_recv()
            c = (i + 1) % 3
            sc[k, c] = (sums[slot, BITS[c] - 1] + rb[k, i].astype(F32)).astype(BF)
            copy("C", c, k).start()

    def finish(k):
        total = mine[k]
        for i in range(3):
            copy("C", i, k).wait_recv()
            total += rc[k, i].astype(F32)
        y_ref[:, pl.ds(pl.multiple_of(k * DC, DC), DC)] = total.astype(BF)

    quick = 2

    @pl.loop(0, nc + 5)
    def _(t):
        @pl.when(t < nc)
        def _():
            project(t)

        kb = jnp.where(t <= quick, t - 1, t - 2)

        @pl.when((t >= 1) & (t != quick + 1) & (t < nc + 2))
        def _():
            stage_b(kb)

        kc = jnp.where(t <= quick + 1, t - 2, t - 3)

        @pl.when((t >= 2) & (t != quick + 2) & (t < nc + 3))
        def _():
            stage_c(kc)

        @pl.when(t < nc)
        def _():
            combine(t)
            shared(t)

        @pl.when(t >= 5)
        def _():
            finish(t - 5)

        @pl.when(t < nc)
        def _():
            stage_a(t)

    @pl.loop(0, nc)
    def _(k):
        @pl.when(k >= nc - 3)
        def _():
            copy("P", 0, k).wait_send()

        for kind in "ABC":
            for i in range(3):
                copy(kind, i, k).wait_send()


def solution(mesh):
    def local(x, expert, slot, gate, w_gate, w_up, w_down, s_gate, s_up, s_down):
        x, expert, slot, gate = x[0, 0], expert[0, 0], slot[0, 0], gate[0, 0]
        tokens, d = x.shape
        top = expert.shape[1]
        experts, _, ff = w_gate.shape
        slots = 5 * tokens * top // (4 * experts * 16)
        rows, nc = 16 * slots, d // DC
        kept = slot < slots
        meta = jnp.concatenate([
            jnp.where(kept, expert, DROPPED).astype(BF).T, jnp.where(kept, slot, 0).astype(BF).T,
            gate.astype(BF).T, jnp.zeros((32 - 3 * top, tokens), BF)], axis=0)
        dma = pltpu.SemaphoreType.DMA
        vmem = pl.BlockSpec(memory_space=pltpu.VMEM)
        hbm = pl.BlockSpec(memory_space=pl.ANY)
        h, hs, cm = pl.pallas_call(
            up_kernel,
            name="up",
            out_shape=[jax.ShapeDtypeStruct((experts, rows, ff), BF),
                       jax.ShapeDtypeStruct((tokens, 2 * ff), BF),
                       jax.ShapeDtypeStruct((16, tokens, 128), BF)],
            in_specs=[vmem, vmem, hbm, hbm, hbm, hbm],
            out_specs=[hbm, hbm, hbm],
            scratch_shapes=[
                pltpu.VMEM((nc, 16, tokens, DC), BF), pltpu.VMEM((16, 32, tokens), BF),
                pltpu.VMEM((16, 128, tokens), BF), pltpu.VMEM((16, tokens, 128), BF),
                pltpu.VMEM((experts, rows, KC), BF),
                pltpu.VMEM((experts, rows, ff), F32), pltpu.VMEM((experts, rows, ff), F32),
                pltpu.VMEM((RING, 2, KC, ff), BF), pltpu.VMEM((2, rows, ff), BF),
                pltpu.VMEM((tokens, 2 * ff), BF),
                dma((nc + 1, 17)), dma((nc + 1, 17)), dma((RING, 2)), dma((4,))],
            compiler_params=pltpu.CompilerParams(
                collective_id=0, has_side_effects=True, vmem_limit_bytes=67_043_328),
        )(x, meta, w_gate, w_up, s_gate, s_up)
        y = pl.pallas_call(
            down_kernel,
            name="down",
            out_shape=jax.ShapeDtypeStruct((tokens, d), BF),
            in_specs=[hbm] * 5,
            out_specs=vmem,
            scratch_shapes=[
                pltpu.VMEM((experts, rows, ff), BF), pltpu.VMEM((tokens, 2 * ff), BF),
                pltpu.VMEM((16, tokens, 128), BF), pltpu.VMEM((RING2, ff, DC), BF),
                pltpu.VMEM((experts, rows, DC), F32), pltpu.VMEM((3, 7, tokens, DC), F32),
                pltpu.VMEM((nc, tokens, DC), F32), pltpu.VMEM((3, 8, tokens, DC), BF),
                pltpu.VMEM((nc, 8, tokens, DC), BF),
                pltpu.VMEM((nc, tokens, DC), BF), pltpu.VMEM((nc, tokens, DC), BF),
                pltpu.VMEM((nc, 3, tokens, DC), BF), pltpu.VMEM((nc, 3, tokens, DC), BF),
                pltpu.VMEM((nc, 3, tokens, DC), BF), pltpu.VMEM((nc, 3, tokens, DC), BF),
                dma((experts + 2,)), dma((RING2,)), dma((nc, 10)), dma((nc, 10))],
            compiler_params=pltpu.CompilerParams(
                collective_id=1, has_side_effects=True, vmem_limit_bytes=67_043_328),
        )(h, hs, cm, w_down, s_down)
        return y[None, None]

    tok = P("dp", "ep", None, None)
    return jax.shard_map(
        local, mesh=mesh,
        in_specs=(tok, tok, tok, tok, P("ep"), P("ep"), P("ep"), P(), P(), P()),
        out_specs=tok, check_vma=False)
```

```python
import functools

import jax
import jax.numpy as jnp
from jax import lax
from jax.experimental import pallas as pl
from jax.experimental.pallas import tpu as pltpu
from jax.sharding import PartitionSpec as P

MESH = pl.DeviceIdType.MESH
BF = jnp.bfloat16
F32 = jnp.float32
DC = 256
BITS = (4, 2, 1)
PARTS = ((0, 96), (96, 80), (176, 80))
REST = (((96, 160),), ((0, 96), (176, 80)), ((0, 176),))
ORDER = (7, 6, 5, 3, 1, 2, 4, 0)
EARLY = tuple((b, rest) for b in range(3) for rest in REST[(b + 2) % 3])
RING = 3
RING2 = 8
KC = 2 * DC
DROPPED = 128


def axes(me):
    def flip(bit):
        return me + bit * (1 - 2 * lax.rem(lax.div(me, bit), 2))

    return [flip(2 * b) for b in BITS], flip(1)


def meet(links, twin):
    barrier = pltpu.get_barrier_semaphore()
    for other in (*links, twin):
        pl.semaphore_signal(barrier, inc=1, device_id={"ep": other}, device_id_type=MESH)
    pl.semaphore_wait(barrier, 4)


def silu_mul(g, u):
    return (g * jax.nn.sigmoid(g) * u).astype(BF)


def up_kernel(x_ref, m_ref, wg, wu, sg, su, h_out, hs_out, cm_out,
              xr, mr, dm, cm, zs, ag, au, wb, hb, hsb, ss, rs, wsem, osem):
    me = lax.axis_index("ep")
    links, twin = axes(me)
    nc = xr.shape[0]
    experts, rows, ff = ag.shape
    tokens = x_ref.shape[0]
    slots = rows // 16
    np_ = nc // 2
    n_shared = 2 * np_
    n_steps = n_shared + np_ * experts

    def start_w(s):
        slot = lax.rem(s, RING)

        @pl.when(s < n_shared)
        def _():
            half, k = lax.div(s, np_), lax.rem(s, np_)
            at = (pl.ds(pl.multiple_of(k * KC, KC), KC), pl.ds(pl.multiple_of(half * ff, ff), ff))
            for i, w in enumerate((sg, su)):
                pltpu.make_async_copy(w.at[at], wb.at[slot, i], wsem.at[slot, i]).start()

        @pl.when((s >= n_shared) & (s < n_steps))
        def _():
            k, e = lax.div(s - n_shared, experts), lax.rem(s - n_shared, experts)
            for i, w in enumerate((wg, wu)):
                src = w.at[e, pl.ds(pl.multiple_of(k * KC, KC), KC), :]
                pltpu.make_async_copy(src, wb.at[slot, i], wsem.at[slot, i]).start()

    def wait_w(s):
        slot = lax.rem(s, RING)
        for i, w in enumerate((wg, wu)):
            pltpu.make_async_copy(w.at[0, pl.ds(0, KC), :], wb.at[slot, i], wsem.at[slot, i]).wait()
        return slot

    for s in range(RING):
        start_w(s)
    meet(links, twin)

    def copy(kind, i, k, turn=0):
        row = nc if k is None else k
        own = m_ref if k is None else x_ref.at[:, pl.ds(pl.multiple_of(k * DC, DC), DC)]

        def block(slot):
            return mr.at[slot] if k is None else xr.at[k, slot]

        if kind == "D":
            src, dst, to, n = own, block(2 * BITS[i]), links[i], i
        elif kind == "F":
            src, dst = block(2 * BITS[(i + 1) % 3]), block(2 * (BITS[i] | BITS[(i + 1) % 3]))
            to, n = links[i], 3 + i
        elif kind == "G":
            src, dst = block(2 * (BITS[(i + 1) % 3] | BITS[(i + 2) % 3])), block(14)
            if k is not None:
                part = pl.ds(*PARTS[(i + turn) % 3])
                src, dst = src.at[part], dst.at[part]
            to, n = links[i], 6 + i
        else:
            src, dst, to, n = own if i == 0 else block(2 * i), block(2 * i + 1), twin, 9 + i
        return pltpu.make_async_remote_copy(
            src_ref=src, dst_ref=dst, send_sem=ss.at[row, n], recv_sem=rs.at[row, n],
            device_id={"ep": to}, device_id_type=MESH)

    def first(k):
        for i in range(3):
            copy("D", i, k).start()

    def second(k):
        for i in range(3):
            copy("D", i, k).wait_recv()
            copy("F", (i + 2) % 3, k).start()
            copy("S", BITS[i], k).start()

    def each(k, do):
        if k is None:
            do(copy("G", 0, None))
            return
        for turn in range(3):
            @pl.when(lax.rem(k, 3) == turn)
            def _():
                for i in range(3):
                    do(copy("G", i, k, turn))

    def third(k):
        for i in range(3):
            copy("F", i, k).wait_recv()
        each(k, lambda c: c.start())
        for i in range(3):
            copy("S", BITS[i] | BITS[(i + 1) % 3], k).start()

    def fourth(k):
        each(k, lambda c: c.wait_recv())
        copy("S", 7, k).start()

    def arrive(k):
        for q in range(8):
            copy("S", q, k).wait_recv()

    def leave(k):
        for kind, count in (("D", 3), ("F", 3), ("S", 8)):
            for i in range(count):
                copy(kind, i, k).wait_send()
        each(k, lambda c: c.wait_send())

    first(None)
    for k in range(2):
        first(k)
    copy("S", 0, None).start()

    @pl.loop(0, nc)
    def _(k):
        copy("S", 0, k).start()
        xr[k, 0] = x_ref[:, pl.ds(pl.multiple_of(k * DC, DC), DC)]

    mr[0] = m_ref[...]

    def matmul(lhs, slot, e, k, emit):
        m = lhs.shape[0]

        def dots(cols):
            return [jnp.dot(lhs, wb[slot, i, :, cols], preferred_element_type=F32) for i in range(2)]

        tiles = [(n, slice(256 * n, 256 * (n + 1))) for n in range(ff // 256)]

        @pl.when(k == 0)
        def _():
            for n, cols in tiles:
                ag[e, :m, cols], au[e, :m, cols] = dots(cols)

        @pl.when((k > 0) & (k < np_ - 1))
        def _():
            for n, cols in tiles:
                g, u = dots(cols)
                ag[e, :m, cols] += g
                au[e, :m, cols] += u

        @pl.when(k == np_ - 1)
        def _():
            for n, cols in tiles:
                g, u = dots(cols)
                emit(n, silu_mul(ag[e, :m, cols] + g, au[e, :m, cols] + u))

    def shared_step(s):
        slot = wait_w(s)
        half, k = lax.div(s, np_), lax.rem(s, np_)

        def emit(n, v):
            hsb[:, pl.ds(pl.multiple_of(half * ff + 256 * n, 256), 256)] = v

        matmul(x_ref[:, pl.ds(pl.multiple_of(k * KC, KC), KC)], slot, 0, k, emit)
        start_w(s + RING)

    def masks():
        base = (me * (experts * slots)).astype(F32)
        row = lax.broadcasted_iota(jnp.int32, (128, tokens), 0)
        want = jnp.where(row < experts * slots, row.astype(F32) + base, -1.0)

        @pl.loop(0, 16)
        def _(d):
            m = mr[d].astype(F32)
            hit = jnp.zeros((128, tokens), F32)
            weight = jnp.zeros((128, tokens), F32)
            for j in range(6):
                place = m[j:j + 1] * float(slots) + m[6 + j:7 + j]
                same = place == want
                hit = jnp.where(same, 1.0, hit)
                weight = jnp.where(same, m[12 + j:13 + j], weight)
            dm[d] = hit.astype(BF)
            cm[d] = weight.T.astype(BF)

    def dispatch(p):
        for half in range(2):
            cols = slice(half * DC, (half + 1) * DC)
            for q in range(8):
                z = [jnp.dot(dm[2 * q + c], xr[2 * p + half, 2 * q + c], preferred_element_type=F32) for c in range(2)]
                for e in range(experts):
                    pair = [v[e * slots:(e + 1) * slots] for v in z]
                    zs[e, 2 * q * slots:2 * (q + 1) * slots, cols] = jnp.concatenate(pair, axis=0).astype(BF)

    def out_copy(e):
        return pltpu.make_async_copy(hb.at[lax.rem(e, 2)], h_out.at[e], osem.at[lax.rem(e, 2)])

    def expert_step(p, e):
        s = n_shared + p * experts + e
        slot = wait_w(s)

        @pl.when((p == np_ - 1) & (e >= 2))
        def _():
            out_copy(e - 2).wait()

        def emit(n, v):
            hb[lax.rem(e, 2), :, 256 * n:256 * (n + 1)] = v

        matmul(zs[e], slot, e, p, emit)
        start_w(s + RING)

        @pl.when(p == np_ - 1)
        def _():
            out_copy(e).start()

    hs_copy = pltpu.make_async_copy(hsb, hs_out, osem.at[2])
    cm_copy = pltpu.make_async_copy(cm, cm_out, osem.at[3])
    split = 2

    @pl.loop(0, nc + 4)
    def _(t):
        for step, do in enumerate((second, third, fourth)):
            @pl.when(t == step)
            def _():
                do(None)

        @pl.when(t < nc)
        def _():
            second(t)

        @pl.when((t >= 1) & (t < nc + 1))
        def _():
            third(t - 1)

        @pl.when(t + 2 < nc)
        def _():
            first(t + 2)

        @pl.when((t >= 2) & (t < nc + 2))
        def _():
            fourth(t - 2)

        @pl.when(t == 3)
        def _():
            hs_copy.start()
            cm_copy.start()

        @pl.when(t < 3)
        def _():
            @pl.loop(0, 4)
            def _(j):
                @pl.when(4 * t + j < n_shared)
                def _():
                    shared_step(4 * t + j)

        @pl.when(t == 2)
        def _():
            arrive(None)
            masks()

        p = lax.div(t - 3, 2)
        early = lax.rem(t, 2) == 1

        @pl.when((t >= 3) & (t < nc + 3) & early)
        def _():
            arrive(2 * p)
            arrive(2 * p + 1)
            dispatch(p)

            @pl.loop(0, split)
            def _(e):
                expert_step(p, e)

        @pl.when((t >= 4) & (t < nc + 4) & ~early)
        def _():
            @pl.loop(split, experts)
            def _(e):
                expert_step(p, e)

    out_copy(experts - 2).wait()
    out_copy(experts - 1).wait()
    hs_copy.wait()
    cm_copy.wait()
    leave(None)

    @pl.loop(0, nc)
    def _(k):
        leave(k)


def down_kernel(h_in, hs_in, cm_in, wd, sd, y_ref, hv, hsv, cmv, wb, os, sums, mine, p1, rd,
                sa, ra, sb, rb, sc, rc, lsem, wsem, ss, rs):
    me = lax.axis_index("ep")
    links, twin = axes(me)
    nc = rd.shape[0]
    experts, rows, ff = hv.shape
    slots = rows // 16
    tokens = y_ref.shape[0]
    tiles = experts + 2
    n_steps = nc * tiles

    def start_w(s):
        slot = lax.rem(s, RING2)
        j, t = lax.div(s, tiles), lax.rem(s, tiles)
        cols = pl.ds(pl.multiple_of(j * DC, DC), DC)

        @pl.when((s < n_steps) & (t < experts))
        def _():
            pltpu.make_async_copy(wd.at[t, :, cols], wb.at[slot], wsem.at[slot]).start()

        @pl.when((s < n_steps) & (t >= experts))
        def _():
            part = pl.ds(pl.multiple_of((t - experts) * ff, ff), ff)
            pltpu.make_async_copy(sd.at[part, cols], wb.at[slot], wsem.at[slot]).start()

    def wait_w(s):
        slot = lax.rem(s, RING2)
        pltpu.make_async_copy(wd.at[0, :, pl.ds(0, DC)], wb.at[slot], wsem.at[slot]).wait()
        return slot

    loads = [pltpu.make_async_copy(h_in.at[e], hv.at[e], lsem.at[e]) for e in range(experts)]
    loads += [pltpu.make_async_copy(cm_in, cmv, lsem.at[experts]),
              pltpu.make_async_copy(hs_in, hsv, lsem.at[experts + 1])]
    for s in range(RING2):
        start_w(s)
        if s < experts + 1:
            loads[s].start()
    loads[experts + 1].start()
    meet(links, twin)

    def copy(kind, i, k):
        if kind == "P":
            part = pl.ds(4 * i, 4)
            src, dst, to, n = p1.at[lax.rem(k, 3), part], rd.at[k, part], twin, 14 * i
        elif kind == "A":
            part = pl.ds(*PARTS[i])
            src, dst, to, n = sa.at[k, part], ra.at[k, part], links[i], 1 + i
        elif kind == "B":
            part = pl.ds(*PARTS[(i + 2) % 3])
            src, dst, to, n = sb.at[k, i, part], rb.at[k, i, part], links[i], 4 + i
        elif kind == "E":
            b, rest = EARLY[i]
            src, dst, to, n = sb.at[k, b, pl.ds(*rest)], rb.at[k, b, pl.ds(*rest)], links[b], 10 + i
        else:
            src, dst, to, n = sc.at[k, i], rc.at[k, i], links[i], 7 + i
        return pltpu.make_async_remote_copy(
            src_ref=src, dst_ref=dst, send_sem=ss.at[k, n], recv_sem=rs.at[k, n],
            device_id={"ep": to}, device_id_type=MESH)

    for c in loads[:experts]:
        c.wait()

    def project(k):
        held = [wait_w(k * tiles + e) for e in range(experts)]
        for e, slot in enumerate(held):
            os[e] = jnp.dot(hv[e], wb[slot], preferred_element_type=F32)
        for e in range(experts):
            start_w(k * tiles + e + RING2)

    def partial(d):
        o = [os[e, d * slots:(d + 1) * slots, :] for e in range(experts)]
        o.append(jnp.zeros((128 - experts * slots, DC), F32))
        return jnp.dot(cmv[d], jnp.concatenate(o, axis=0).astype(BF), preferred_element_type=F32)

    def combine(k):
        slot = lax.rem(k, 3)

        @pl.when(k >= 3)
        def _():
            for half in range(2):
                copy("P", half, k - 3).wait_send()

        for half in range(2):
            for n in range(4 * half, 4 * half + 4):
                p1[slot, n] = partial(2 * ORDER[n] + 1).astype(BF)
            copy("P", half, k).start()

        for q in range(1, 8):
            sums[slot, q - 1] = partial(2 * q)

        mine[k] = partial(0)

    def shared(k):
        held = [wait_w(k * tiles + experts + half) for half in range(2)]
        mine[k] += sum(jnp.dot(hsv[:, half * ff:(half + 1) * ff], wb[slot], preferred_element_type=F32)
                       for half, slot in enumerate(held))
        for half in range(2):
            start_w(k * tiles + experts + half + RING2)

    def stage_a(k):
        slot = lax.rem(k, 3)

        def other(q):
            return rd[k, ORDER.index(q)].astype(F32)

        copy("P", 0, k).wait_recv()
        sa[k] = (sums[slot, 6] + other(7)).astype(BF)
        for i in range(3):
            copy("A", i, k).start()
        for b in range(3):
            q = 7 ^ BITS[(b + 2) % 3]
            sums[slot, q - 1] += other(q)
            for n, (owner, (start, size)) in enumerate(EARLY):
                if owner == b:
                    rest = slice(start, start + size)
                    sb[k, b, rest] = sums[slot, q - 1, rest].astype(BF)
                    copy("E", n, k).start()
        copy("P", 1, k).wait_recv()
        for q in (1, 2, 4):
            sums[slot, q - 1] += other(q)
        mine[k] += other(0)

    def stage_b(k):
        slot = lax.rem(k, 3)
        for i in range(3):
            copy("A", i, k).wait_recv()
            b, q = (i + 1) % 3, 7 ^ BITS[i]
            part = slice(PARTS[i][0], PARTS[i][0] + PARTS[i][1])
            sb[k, b, part] = (sums[slot, q - 1, part] + ra[k, part].astype(F32)).astype(BF)
            copy("B", b, k).start()

    def stage_c(k):
        slot = lax.rem(k, 3)
        for i in range(3):
            for n, (owner, rest) in enumerate(EARLY):
                if owner == i:
                    copy("E", n, k).wait_recv()
            copy("B", i, k).wait_recv()
            c = (i + 1) % 3
            sc[k, c] = (sums[slot, BITS[c] - 1] + rb[k, i].astype(F32)).astype(BF)
            copy("C", c, k).start()

    def finish(k):
        total = mine[k]
        for i in range(3):
            copy("C", i, k).wait_recv()
            total += rc[k, i].astype(F32)
        y_ref[:, pl.ds(pl.multiple_of(k * DC, DC), DC)] = total.astype(BF)

    quick = 2

    @pl.loop(0, nc + 5)
    def _(t):
        @pl.when(t < nc)
        def _():
            project(t)

        kb = jnp.where(t <= quick, t - 1, t - 2)

        @pl.when((t >= 1) & (t != quick + 1) & (t < nc + 2))
        def _():
            stage_b(kb)

        kc = jnp.where(t <= quick + 1, t - 2, t - 3)

        @pl.when((t >= 2) & (t != quick + 2) & (t < nc + 3))
        def _():
            stage_c(kc)

        @pl.when(t == 0)
        def _():
            loads[experts].wait()

        @pl.when(t < nc)
        def _():
            combine(t)

        @pl.when(t == 0)
        def _():
            stage_a(t)
            loads[experts + 1].wait()

        @pl.when(t < nc)
        def _():
            shared(t)

        @pl.when(t >= 5)
        def _():
            finish(t - 5)

        @pl.when((t > 0) & (t < nc))
        def _():
            stage_a(t)

    @pl.loop(0, nc)
    def _(k):
        @pl.when(k >= nc - 3)
        def _():
            for half in range(2):
                copy("P", half, k).wait_send()

        for kind, count in (("A", 3), ("B", 3), ("C", 3), ("E", len(EARLY))):
            for i in range(count):
                copy(kind, i, k).wait_send()


def solution(mesh):
    def local(x, expert, slot, gate, w_gate, w_up, w_down, s_gate, s_up, s_down):
        x, expert, slot, gate = x[0, 0], expert[0, 0], slot[0, 0], gate[0, 0]
        tokens, d = x.shape
        top = expert.shape[1]
        experts, _, ff = w_gate.shape
        slots = 5 * tokens * top // (4 * experts * 16)
        rows, nc = 16 * slots, d // DC
        kept = slot < slots
        meta = jnp.concatenate([
            jnp.where(kept, expert, DROPPED).astype(BF).T, jnp.where(kept, slot, 0).astype(BF).T,
            gate.astype(BF).T, jnp.zeros((32 - 3 * top, tokens), BF)], axis=0)
        dma = pltpu.SemaphoreType.DMA
        vmem = pl.BlockSpec(memory_space=pltpu.VMEM)
        hbm = pl.BlockSpec(memory_space=pl.ANY)
        h, hs, cm = pl.pallas_call(
            up_kernel,
            name="up",
            out_shape=[jax.ShapeDtypeStruct((experts, rows, ff), BF),
                       jax.ShapeDtypeStruct((tokens, 2 * ff), BF),
                       jax.ShapeDtypeStruct((16, tokens, 128), BF)],
            in_specs=[vmem, vmem, hbm, hbm, hbm, hbm],
            out_specs=[hbm, hbm, hbm],
            scratch_shapes=[
                pltpu.VMEM((nc, 16, tokens, DC), BF), pltpu.VMEM((16, 32, tokens), BF),
                pltpu.VMEM((16, 128, tokens), BF), pltpu.VMEM((16, tokens, 128), BF),
                pltpu.VMEM((experts, rows, KC), BF),
                pltpu.VMEM((experts, rows, ff), F32), pltpu.VMEM((experts, rows, ff), F32),
                pltpu.VMEM((RING, 2, KC, ff), BF), pltpu.VMEM((2, rows, ff), BF),
                pltpu.VMEM((tokens, 2 * ff), BF),
                dma((nc + 1, 17)), dma((nc + 1, 17)), dma((RING, 2)), dma((4,))],
            compiler_params=pltpu.CompilerParams(
                collective_id=0, has_side_effects=True, vmem_limit_bytes=67_043_328),
        )(x, meta, w_gate, w_up, s_gate, s_up)
        y = pl.pallas_call(
            down_kernel,
            name="down",
            out_shape=jax.ShapeDtypeStruct((tokens, d), BF),
            in_specs=[hbm] * 5,
            out_specs=vmem,
            scratch_shapes=[
                pltpu.VMEM((experts, rows, ff), BF), pltpu.VMEM((tokens, 2 * ff), BF),
                pltpu.VMEM((16, tokens, 128), BF), pltpu.VMEM((RING2, ff, DC), BF),
                pltpu.VMEM((experts, rows, DC), F32), pltpu.VMEM((3, 7, tokens, DC), F32),
                pltpu.VMEM((nc, tokens, DC), F32), pltpu.VMEM((3, 8, tokens, DC), BF),
                pltpu.VMEM((nc, 8, tokens, DC), BF),
                pltpu.VMEM((nc, tokens, DC), BF), pltpu.VMEM((nc, tokens, DC), BF),
                pltpu.VMEM((nc, 3, tokens, DC), BF), pltpu.VMEM((nc, 3, tokens, DC), BF),
                pltpu.VMEM((nc, 3, tokens, DC), BF), pltpu.VMEM((nc, 3, tokens, DC), BF),
                dma((experts + 2,)), dma((RING2,)), dma((nc, 15)), dma((nc, 15))],
            compiler_params=pltpu.CompilerParams(
                collective_id=1, has_side_effects=True, vmem_limit_bytes=67_043_328),
        )(h, hs, cm, w_down, s_down)
        return y[None, None]

    tok = P("dp", "ep", None, None)
    return jax.shard_map(
        local, mesh=mesh,
        in_specs=(tok, tok, tok, tok, P("ep"), P("ep"), P("ep"), P(), P(), P()),
        out_specs=tok, check_vma=False)
```

```python
import functools

import jax
import jax.numpy as jnp
from jax import lax
from jax.experimental import pallas as pl
from jax.experimental.pallas import tpu as pltpu
from jax.sharding import PartitionSpec as P

MESH = pl.DeviceIdType.MESH
BF = jnp.bfloat16
F32 = jnp.float32
DC = 256
BITS = (4, 2, 1)
PARTS = ((0, 96), (96, 80), (176, 80))
REST = (((96, 160),), ((0, 96), (176, 80)), ((0, 176),))
ORDER = (7, 6, 5, 3, 1, 2, 4, 0)
EARLY = [[(b, rest) for b in range(3) for rest in REST[(b + 2 + turn) % 3]] for turn in range(3)]
RING = 3
RING2 = 8
KC = 2 * DC
DROPPED = 128


def axes(me):
    def flip(bit):
        return me + bit * (1 - 2 * lax.rem(lax.div(me, bit), 2))

    return [flip(2 * b) for b in BITS], flip(1)


def meet(links, twin):
    barrier = pltpu.get_barrier_semaphore()
    for other in (*links, twin):
        pl.semaphore_signal(barrier, inc=1, device_id={"ep": other}, device_id_type=MESH)
    pl.semaphore_wait(barrier, 4)


def silu_mul(g, u):
    return (g * jax.nn.sigmoid(g) * u).astype(BF)


def up_kernel(x_ref, m_ref, wg, wu, sg, su, h_out, hs_out, cm_out,
              xr, mr, dm, cm, zs, ag, au, wb, hb, hsb, ss, rs, wsem, osem):
    me = lax.axis_index("ep")
    links, twin = axes(me)
    nc = xr.shape[0]
    experts, rows, ff = ag.shape
    tokens = x_ref.shape[0]
    slots = rows // 16
    np_ = nc // 2
    n_shared = 2 * np_
    n_steps = n_shared + np_ * experts

    def start_w(s):
        slot = lax.rem(s, RING)

        @pl.when(s < n_shared)
        def _():
            half, k = lax.div(s, np_), lax.rem(s, np_)
            at = (pl.ds(pl.multiple_of(k * KC, KC), KC), pl.ds(pl.multiple_of(half * ff, ff), ff))
            for i, w in enumerate((sg, su)):
                pltpu.make_async_copy(w.at[at], wb.at[slot, i], wsem.at[slot, i]).start()

        @pl.when((s >= n_shared) & (s < n_steps))
        def _():
            k, e = lax.div(s - n_shared, experts), lax.rem(s - n_shared, experts)
            for i, w in enumerate((wg, wu)):
                src = w.at[e, pl.ds(pl.multiple_of(k * KC, KC), KC), :]
                pltpu.make_async_copy(src, wb.at[slot, i], wsem.at[slot, i]).start()

    def wait_w(s):
        slot = lax.rem(s, RING)
        for i, w in enumerate((wg, wu)):
            pltpu.make_async_copy(w.at[0, pl.ds(0, KC), :], wb.at[slot, i], wsem.at[slot, i]).wait()
        return slot

    for s in range(RING):
        start_w(s)
    meet(links, twin)

    def copy(kind, i, k, turn=0):
        row = nc if k is None else k
        own = m_ref if k is None else x_ref.at[:, pl.ds(pl.multiple_of(k * DC, DC), DC)]

        def block(slot):
            return mr.at[slot] if k is None else xr.at[k, slot]

        if kind == "D":
            src, dst, to, n = own, block(2 * BITS[i]), links[i], i
        elif kind == "F":
            src, dst = block(2 * BITS[(i + 1) % 3]), block(2 * (BITS[i] | BITS[(i + 1) % 3]))
            to, n = links[i], 3 + i
        elif kind == "G":
            src, dst = block(2 * (BITS[(i + 1) % 3] | BITS[(i + 2) % 3])), block(14)
            if k is not None:
                part = pl.ds(*PARTS[(i + turn) % 3])
                src, dst = src.at[part], dst.at[part]
            to, n = links[i], 6 + i
        else:
            src, dst, to, n = own if i == 0 else block(2 * i), block(2 * i + 1), twin, 9 + i
        return pltpu.make_async_remote_copy(
            src_ref=src, dst_ref=dst, send_sem=ss.at[row, n], recv_sem=rs.at[row, n],
            device_id={"ep": to}, device_id_type=MESH)

    def first(k):
        for i in range(3):
            copy("D", i, k).start()

    def second(k):
        for i in range(3):
            copy("D", i, k).wait_recv()
            copy("F", (i + 2) % 3, k).start()
            copy("S", BITS[i], k).start()

    def each(k, do):
        if k is None:
            do(copy("G", 0, None))
            return
        for turn in range(3):
            @pl.when(lax.rem(k, 3) == turn)
            def _():
                for i in range(3):
                    do(copy("G", i, k, turn))

    def third(k):
        for i in range(3):
            copy("F", i, k).wait_recv()
        each(k, lambda c: c.start())
        for i in range(3):
            copy("S", BITS[i] | BITS[(i + 1) % 3], k).start()

    def fourth(k):
        each(k, lambda c: c.wait_recv())
        copy("S", 7, k).start()

    def arrive(k):
        for q in range(8):
            copy("S", q, k).wait_recv()

    def leave(k):
        for kind, count in (("D", 3), ("F", 3), ("S", 8)):
            for i in range(count):
                copy(kind, i, k).wait_send()
        each(k, lambda c: c.wait_send())

    first(None)
    for k in range(2):
        first(k)
    copy("S", 0, None).start()

    @pl.loop(0, nc)
    def _(k):
        copy("S", 0, k).start()
        xr[k, 0] = x_ref[:, pl.ds(pl.multiple_of(k * DC, DC), DC)]

    mr[0] = m_ref[...]

    def matmul(lhs, slot, e, k, emit):
        m = lhs.shape[0]

        def dots(cols):
            return [jnp.dot(lhs, wb[slot, i, :, cols], preferred_element_type=F32) for i in range(2)]

        tiles = [(n, slice(256 * n, 256 * (n + 1))) for n in range(ff // 256)]

        @pl.when(k == 0)
        def _():
            for n, cols in tiles:
                ag[e, :m, cols], au[e, :m, cols] = dots(cols)

        @pl.when((k > 0) & (k < np_ - 1))
        def _():
            for n, cols in tiles:
                g, u = dots(cols)
                ag[e, :m, cols] += g
                au[e, :m, cols] += u

        @pl.when(k == np_ - 1)
        def _():
            for n, cols in tiles:
                g, u = dots(cols)
                emit(n, silu_mul(ag[e, :m, cols] + g, au[e, :m, cols] + u))

    def shared_step(s):
        slot = wait_w(s)
        half, k = lax.div(s, np_), lax.rem(s, np_)

        def emit(n, v):
            hsb[:, pl.ds(pl.multiple_of(half * ff + 256 * n, 256), 256)] = v

        matmul(x_ref[:, pl.ds(pl.multiple_of(k * KC, KC), KC)], slot, 0, k, emit)
        start_w(s + RING)

    def masks():
        base = (me * (experts * slots)).astype(F32)
        row = lax.broadcasted_iota(jnp.int32, (128, tokens), 0)
        want = jnp.where(row < experts * slots, row.astype(F32) + base, -1.0)

        @pl.loop(0, 16)
        def _(d):
            m = mr[d].astype(F32)
            hit = jnp.zeros((128, tokens), F32)
            weight = jnp.zeros((128, tokens), F32)
            for j in range(6):
                place = m[j:j + 1] * float(slots) + m[6 + j:7 + j]
                same = place == want
                hit = jnp.where(same, 1.0, hit)
                weight = jnp.where(same, m[12 + j:13 + j], weight)
            dm[d] = hit.astype(BF)
            cm[d] = weight.T.astype(BF)

    def dispatch(p):
        for half in range(2):
            cols = slice(half * DC, (half + 1) * DC)
            for q in range(8):
                z = [jnp.dot(dm[2 * q + c], xr[2 * p + half, 2 * q + c], preferred_element_type=F32) for c in range(2)]
                for e in range(experts):
                    pair = [v[e * slots:(e + 1) * slots] for v in z]
                    zs[e, 2 * q * slots:2 * (q + 1) * slots, cols] = jnp.concatenate(pair, axis=0).astype(BF)

    def out_copy(e):
        return pltpu.make_async_copy(hb.at[lax.rem(e, 2)], h_out.at[e], osem.at[lax.rem(e, 2)])

    def expert_step(p, e):
        s = n_shared + p * experts + e
        slot = wait_w(s)

        @pl.when((p == np_ - 1) & (e >= 2))
        def _():
            out_copy(e - 2).wait()

        def emit(n, v):
            hb[lax.rem(e, 2), :, 256 * n:256 * (n + 1)] = v

        matmul(zs[e], slot, e, p, emit)
        start_w(s + RING)

        @pl.when(p == np_ - 1)
        def _():
            out_copy(e).start()

    hs_copy = pltpu.make_async_copy(hsb, hs_out, osem.at[2])
    cm_copy = pltpu.make_async_copy(cm, cm_out, osem.at[3])
    split = 3

    @pl.loop(0, nc + 4)
    def _(t):
        for step, do in enumerate((second, third, fourth)):
            @pl.when(t == step)
            def _():
                do(None)

        @pl.when(t < nc)
        def _():
            second(t)

        @pl.when((t >= 1) & (t < nc + 1))
        def _():
            third(t - 1)

        @pl.when(t + 2 < nc)
        def _():
            first(t + 2)

        @pl.when((t >= 2) & (t < nc + 2))
        def _():
            fourth(t - 2)

        @pl.when(t == 3)
        def _():
            hs_copy.start()
            cm_copy.start()

        @pl.when(t < 3)
        def _():
            @pl.loop(0, 4)
            def _(j):
                @pl.when(4 * t + j < n_shared)
                def _():
                    shared_step(4 * t + j)

        @pl.when(t == 2)
        def _():
            arrive(None)
            masks()

        p = lax.div(t - 3, 2)
        early = lax.rem(t, 2) == 1

        @pl.when((t >= 3) & (t < nc + 3) & early)
        def _():
            arrive(2 * p)
            arrive(2 * p + 1)
            dispatch(p)

            @pl.loop(0, split)
            def _(e):
                expert_step(p, e)

        @pl.when((t >= 4) & (t < nc + 4) & ~early)
        def _():
            @pl.loop(split, experts)
            def _(e):
                expert_step(p, e)

    out_copy(experts - 2).wait()
    out_copy(experts - 1).wait()
    hs_copy.wait()
    cm_copy.wait()
    leave(None)

    @pl.loop(0, nc)
    def _(k):
        leave(k)


def down_kernel(h_in, hs_in, cm_in, wd, sd, y_ref, hv, hsv, cmv, wb, os, sums, mine, p1, rd,
                sa, ra, sb, rb, sc, rc, lsem, wsem, ss, rs):
    me = lax.axis_index("ep")
    links, twin = axes(me)
    nc = rd.shape[0]
    experts, rows, ff = hv.shape
    slots = rows // 16
    tokens = y_ref.shape[0]
    tiles = experts + 2
    n_steps = nc * tiles

    def start_w(s):
        slot = lax.rem(s, RING2)
        j, t = lax.div(s, tiles), lax.rem(s, tiles)
        cols = pl.ds(pl.multiple_of(j * DC, DC), DC)

        @pl.when((s < n_steps) & (t < experts))
        def _():
            pltpu.make_async_copy(wd.at[t, :, cols], wb.at[slot], wsem.at[slot]).start()

        @pl.when((s < n_steps) & (t >= experts))
        def _():
            part = pl.ds(pl.multiple_of((t - experts) * ff, ff), ff)
            pltpu.make_async_copy(sd.at[part, cols], wb.at[slot], wsem.at[slot]).start()

    def wait_w(s):
        slot = lax.rem(s, RING2)
        pltpu.make_async_copy(wd.at[0, :, pl.ds(0, DC)], wb.at[slot], wsem.at[slot]).wait()
        return slot

    loads = [pltpu.make_async_copy(h_in.at[e], hv.at[e], lsem.at[e]) for e in range(experts)]
    loads += [pltpu.make_async_copy(cm_in, cmv, lsem.at[experts]),
              pltpu.make_async_copy(hs_in, hsv, lsem.at[experts + 1])]
    for s in range(RING2):
        start_w(s)
        if s < experts + 1:
            loads[s].start()
    loads[experts + 1].start()
    meet(links, twin)

    def by_turns(k, do):
        for turn in range(3):
            @pl.when(lax.rem(k, 3) == turn)
            def _():
                do(k, turn)

    def copy(kind, i, k, turn=0):
        if kind == "P":
            part = pl.ds(4 * i, 4)
            src, dst, to, n = p1.at[lax.rem(k, 3), part], rd.at[k, part], twin, 14 * i
        elif kind == "A":
            part = pl.ds(*PARTS[(i + turn) % 3])
            src, dst, to, n = sa.at[k, part], ra.at[k, part], links[i], 1 + i
        elif kind == "B":
            part = pl.ds(*PARTS[(i + 2 + turn) % 3])
            src, dst, to, n = sb.at[k, i, part], rb.at[k, i, part], links[i], 4 + i
        elif kind == "E":
            b, rest = EARLY[turn][i]
            src, dst, to, n = sb.at[k, b, pl.ds(*rest)], rb.at[k, b, pl.ds(*rest)], links[b], 10 + i
        else:
            src, dst, to, n = sc.at[k, i], rc.at[k, i], links[i], 7 + i
        return pltpu.make_async_remote_copy(
            src_ref=src, dst_ref=dst, send_sem=ss.at[k, n], recv_sem=rs.at[k, n],
            device_id={"ep": to}, device_id_type=MESH)

    def project(k):
        held = [wait_w(k * tiles + e) for e in range(experts)]
        for e, slot in enumerate(held):
            os[e] = jnp.dot(hv[e], wb[slot], preferred_element_type=F32)
        for e in range(experts):
            start_w(k * tiles + e + RING2)

    for e in range(experts):
        loads[e].wait()
        os[e] = jnp.dot(hv[e], wb[wait_w(e)], preferred_element_type=F32)
        start_w(e + RING2)
    loads[experts].wait()

    def partial(d):
        o = [os[e, d * slots:(d + 1) * slots, :] for e in range(experts)]
        o.append(jnp.zeros((128 - experts * slots, DC), F32))
        return jnp.dot(cmv[d], jnp.concatenate(o, axis=0).astype(BF), preferred_element_type=F32)

    def combine(k):
        slot = lax.rem(k, 3)

        @pl.when(k >= 3)
        def _():
            for half in range(2):
                copy("P", half, k - 3).wait_send()

        for half in range(2):
            for n in range(4 * half, 4 * half + 4):
                p1[slot, n] = partial(2 * ORDER[n] + 1).astype(BF)
            copy("P", half, k).start()

        for q in range(1, 8):
            sums[slot, q - 1] = partial(2 * q)

        mine[k] = partial(0)

    def shared(k):
        held = [wait_w(k * tiles + experts + half) for half in range(2)]
        mine[k] += sum(jnp.dot(hsv[:, half * ff:(half + 1) * ff], wb[slot], preferred_element_type=F32)
                       for half, slot in enumerate(held))
        for half in range(2):
            start_w(k * tiles + experts + half + RING2)

    def stage_a(k, turn):
        slot = lax.rem(k, 3)

        def other(q):
            return rd[k, ORDER.index(q)].astype(F32)

        copy("P", 0, k).wait_recv()
        sa[k] = (sums[slot, 6] + other(7)).astype(BF)
        for i in range(3):
            copy("A", i, k, turn).start()
        for b in range(3):
            q = 7 ^ BITS[(b + 2) % 3]
            sums[slot, q - 1] += other(q)
            for n, (owner, (start, size)) in enumerate(EARLY[turn]):
                if owner == b:
                    rest = slice(start, start + size)
                    sb[k, b, rest] = sums[slot, q - 1, rest].astype(BF)
                    copy("E", n, k, turn).start()
        copy("P", 1, k).wait_recv()
        for q in (1, 2, 4):
            sums[slot, q - 1] += other(q)
        mine[k] += other(0)

    def stage_b(k, turn):
        slot = lax.rem(k, 3)
        for i in range(3):
            copy("A", i, k, turn).wait_recv()
            b, q = (i + 1) % 3, 7 ^ BITS[i]
            start, size = PARTS[(i + turn) % 3]
            part = slice(start, start + size)
            sb[k, b, part] = (sums[slot, q - 1, part] + ra[k, part].astype(F32)).astype(BF)
            copy("B", b, k, turn).start()

    def stage_c(k, turn):
        slot = lax.rem(k, 3)
        for i in range(3):
            for n, (owner, rest) in enumerate(EARLY[turn]):
                if owner == i:
                    copy("E", n, k, turn).wait_recv()
            copy("B", i, k, turn).wait_recv()
            c = (i + 1) % 3
            sc[k, c] = (sums[slot, BITS[c] - 1] + rb[k, i].astype(F32)).astype(BF)
            copy("C", c, k).start()

    def finish(k):
        total = mine[k]
        for i in range(3):
            copy("C", i, k).wait_recv()
            total += rc[k, i].astype(F32)
        y_ref[:, pl.ds(pl.multiple_of(k * DC, DC), DC)] = total.astype(BF)

    quick = 2

    @pl.loop(0, nc + 5)
    def _(t):
        @pl.when((t > 0) & (t < nc))
        def _():
            project(t)

        kb = jnp.where(t <= quick, t - 1, t - 2)

        @pl.when((t >= 1) & (t != quick + 1) & (t < nc + 2))
        def _():
            by_turns(kb, stage_b)

        kc = jnp.where(t <= quick + 1, t - 2, t - 3)

        @pl.when((t >= 2) & (t != quick + 2) & (t < nc + 3))
        def _():
            by_turns(kc, stage_c)

        @pl.when(t < nc)
        def _():
            combine(t)

        @pl.when(t == 0)
        def _():
            stage_a(t, 0)
            loads[experts + 1].wait()

        @pl.when(t < nc)
        def _():
            shared(t)

        @pl.when(t >= 5)
        def _():
            finish(t - 5)

        @pl.when((t > 0) & (t < nc))
        def _():
            by_turns(t, stage_a)

    @pl.loop(0, nc)
    def _(k):
        @pl.when(k >= nc - 3)
        def _():
            for half in range(2):
                copy("P", half, k).wait_send()

        def leave(k, turn):
            for kind, count in (("A", 3), ("B", 3), ("C", 3), ("E", 4)):
                for i in range(count):
                    copy(kind, i, k, turn).wait_send()

        by_turns(k, leave)


def solution(mesh):
    def local(x, expert, slot, gate, w_gate, w_up, w_down, s_gate, s_up, s_down):
        x, expert, slot, gate = x[0, 0], expert[0, 0], slot[0, 0], gate[0, 0]
        tokens, d = x.shape
        top = expert.shape[1]
        experts, _, ff = w_gate.shape
        slots = 5 * tokens * top // (4 * experts * 16)
        rows, nc = 16 * slots, d // DC
        kept = slot < slots
        meta = jnp.concatenate([
            jnp.where(kept, expert, DROPPED).astype(BF).T, jnp.where(kept, slot, 0).astype(BF).T,
            gate.astype(BF).T, jnp.zeros((32 - 3 * top, tokens), BF)], axis=0)
        dma = pltpu.SemaphoreType.DMA
        vmem = pl.BlockSpec(memory_space=pltpu.VMEM)
        hbm = pl.BlockSpec(memory_space=pl.ANY)
        h, hs, cm = pl.pallas_call(
            up_kernel,
            name="up",
            out_shape=[jax.ShapeDtypeStruct((experts, rows, ff), BF),
                       jax.ShapeDtypeStruct((tokens, 2 * ff), BF),
                       jax.ShapeDtypeStruct((16, tokens, 128), BF)],
            in_specs=[vmem, vmem, hbm, hbm, hbm, hbm],
            out_specs=[hbm, hbm, hbm],
            scratch_shapes=[
                pltpu.VMEM((nc, 16, tokens, DC), BF), pltpu.VMEM((16, 32, tokens), BF),
                pltpu.VMEM((16, 128, tokens), BF), pltpu.VMEM((16, tokens, 128), BF),
                pltpu.VMEM((experts, rows, KC), BF),
                pltpu.VMEM((experts, rows, ff), F32), pltpu.VMEM((experts, rows, ff), F32),
                pltpu.VMEM((RING, 2, KC, ff), BF), pltpu.VMEM((2, rows, ff), BF),
                pltpu.VMEM((tokens, 2 * ff), BF),
                dma((nc + 1, 17)), dma((nc + 1, 17)), dma((RING, 2)), dma((4,))],
            compiler_params=pltpu.CompilerParams(
                collective_id=0, has_side_effects=True, vmem_limit_bytes=67_043_328),
        )(x, meta, w_gate, w_up, s_gate, s_up)
        y = pl.pallas_call(
            down_kernel,
            name="down",
            out_shape=jax.ShapeDtypeStruct((tokens, d), BF),
            in_specs=[hbm] * 5,
            out_specs=vmem,
            scratch_shapes=[
                pltpu.VMEM((experts, rows, ff), BF), pltpu.VMEM((tokens, 2 * ff), BF),
                pltpu.VMEM((16, tokens, 128), BF), pltpu.VMEM((RING2, ff, DC), BF),
                pltpu.VMEM((experts, rows, DC), F32), pltpu.VMEM((3, 7, tokens, DC), F32),
                pltpu.VMEM((nc, tokens, DC), F32), pltpu.VMEM((3, 8, tokens, DC), BF),
                pltpu.VMEM((nc, 8, tokens, DC), BF),
                pltpu.VMEM((nc, tokens, DC), BF), pltpu.VMEM((nc, tokens, DC), BF),
                pltpu.VMEM((nc, 3, tokens, DC), BF), pltpu.VMEM((nc, 3, tokens, DC), BF),
                pltpu.VMEM((nc, 3, tokens, DC), BF), pltpu.VMEM((nc, 3, tokens, DC), BF),
                dma((experts + 2,)), dma((RING2,)), dma((nc, 15)), dma((nc, 15))],
            compiler_params=pltpu.CompilerParams(
                collective_id=1, has_side_effects=True, vmem_limit_bytes=67_043_328),
        )(h, hs, cm, w_down, s_down)
        return y[None, None]

    tok = P("dp", "ep", None, None)
    return jax.shard_map(
        local, mesh=mesh,
        in_specs=(tok, tok, tok, tok, P("ep"), P("ep"), P("ep"), P(), P(), P()),
        out_specs=tok, check_vma=False)
```
